32 devices in a mesh: rows: 8 (over z, y), grp: 4 (over x, core).
Axes of the slice: x: 2, y: 2, z: 4, core: 2. Of those that a mesh axis runs over, the one named last changes fastest.
Arguments:
- features: float32 [8192, 128], P(('rows', 'grp'))
- key_ids: int32 [8192], P(('rows', 'grp')), may hold values from 0 to 23, as said below
- owner: int32 [24], replicated, may hold values from 0 to 23, each once
Outputs:
- covariance: float32 [3072, 128], P(('rows', 'grp'))
The draws below stay inside these ranges and needn't reach their ends.
Inputs may be any that keep to these rules, and one draw needn't show every extreme that they name: `key_ids`: every key is the key of at least 2 rows.
All inputs are finite; a program needn't handle non-finite values.
Results may differ from the reference program's by a relative error of at most 0.0003.
Values sent between devices are 32-bit elements; how exact they have to be, the bound alone decides.
A program may use at most 64 MiB of HBM per device.

```python
import math
import jax
import jax.numpy as jnp
from jax import lax

F = 128
KEYS = 24
ROWS = 8192


def draw_key_ids(key, part):
    first, second, third = jax.random.split(jax.random.fold_in(key, 11), 3)
    left = jax.random.randint(first, (ROWS,), 0, KEYS)
    right = jax.random.randint(second, (ROWS,), 0, KEYS)
    ranked = left * right // KEYS
    order = jax.random.permutation(third, KEYS)
    chosen = order[ranked]
    position = jnp.arange(ROWS, dtype=jnp.int32)
    chosen = jnp.where(position < 2 * KEYS, position % KEYS, chosen)
    return chosen.astype(jnp.int32)


def draw_features(key, part):
    first, second = jax.random.split(jax.random.fold_in(key, 23), 2)
    offsets = jax.random.uniform(second, (1, F), jnp.float32, -3.0, 3.0)
    values = jax.random.normal(first, (ROWS, F), jnp.float32)
    return (values + offsets).astype(jnp.float32)


def setup_inputs(seed: int = 0) -> dict:
    arg_keys = jax.random.split(jax.random.key(seed), 4)
    features = draw_features(jax.random.fold_in(arg_keys[3], 71), 0)
    key_ids = draw_key_ids(jax.random.fold_in(arg_keys[3], 71), 0)
    owner = jax.random.permutation(arg_keys[2], KEYS).astype(jnp.int32)
    return dict(features=features, key_ids=key_ids, owner=owner)


def reference(features, key_ids, owner):
    slot = owner[key_ids].astype(jnp.int32)
    count = jax.ops.segment_sum(jnp.ones((ROWS,), jnp.float32), slot, KEYS)
    total = jax.ops.segment_sum(features, slot, KEYS)
    block = math.gcd(ROWS, 1024)
    steps = ROWS // block

    def accumulate(acc, index):
        start = (index * block).astype(jnp.int32)
        piece = lax.dynamic_slice_in_dim(features, start, block, 0)
        labels = lax.dynamic_slice_in_dim(slot, start, block, 0)
        outer = piece[:, :, None] * piece[:, None, :]
        return acc + jax.ops.segment_sum(outer, labels, KEYS), None

    gram, _ = lax.scan(accumulate, jnp.zeros((KEYS, F, F), jnp.float32), jnp.arange(steps, dtype=jnp.int32))
    centred = gram - total[:, :, None] * total[:, None, :] / count[:, None, None]
    result = centred / (count - 1.0)[:, None, None]
    return result.reshape(KEYS * F, F)
```

```python
import functools

import jax
import jax.numpy as jnp
from jax import lax
from jax.experimental import pallas as pl
from jax.experimental.pallas import tpu as pltpu
from jax.sharding import PartitionSpec as P

MESH = pl.DeviceIdType.MESH
LANES = 128
TAIL = 8


def flip(q, mask):
    bit = 1
    while bit <= mask:
        if mask & bit:
            q = q + bit * (1 - 2 * ((q // bit) % 2))
        bit *= 2
    return q


def kernel(
    inner, n_grp, n_line, nkeys, length, padded,
    feat_ref, key_ref, owner_ref, out_ref,
    blocks, keys, part, arrived, load_sem, send_sem, recv_sem, line_send, line_recv,
):
    group = inner * n_grp
    nrows, width = feat_ref.shape
    r, g = lax.axis_index("rows"), lax.axis_index("grp")
    line = r // inner
    q = (r % inner) * n_grp + g

    def peer(mask):
        other = flip(q, mask)
        return (line * inner + other // n_grp, other % n_grp)

    def along(step):
        return (((line + step) % n_line) * inner + r % inner, g)

    loads = [
        pltpu.make_async_copy(feat_ref, blocks.at[0], load_sem.at[0]),
        pltpu.make_async_copy(key_ref, keys.at[0], load_sem.at[1]),
    ]
    for copy in loads:
        copy.start()
    far = list(range(2, group, 2))
    barrier = pltpu.get_barrier_semaphore()
    for mask in [1] + far:
        pl.semaphore_signal(barrier, inc=1, device_id=peer(mask), device_id_type=MESH)
    if n_line <= 8:
        for step in range(1, n_line):
            pl.semaphore_signal(barrier, inc=1, device_id=along(step), device_id_type=MESH)
    else:
        def greet(step, c):
            pl.semaphore_signal(barrier, inc=1, device_id=along(step), device_id_type=MESH)
            return c
        lax.fori_loop(1, n_line, greet, 0)

    lane = lax.broadcasted_iota(jnp.int32, (1, LANES), 1)
    inverse = jnp.zeros((1, LANES), jnp.int32)
    for k in range(nkeys):
        inverse = jnp.where(lane == owner_ref[k], k + 1, inverse)
    row = lax.broadcasted_iota(jnp.int32, (padded + TAIL, 1), 0)

    def base_of(step):
        return (((line + step) % n_line) * group + q) * length

    def wanted(step):
        base = base_of(step)
        tail = (row - padded) % (TAIL // 2)
        slot = jnp.where(row < padded, (base + row) // width, base // width + tail)
        last = (base + length - 1) // width
        none = ((row >= length) & (row < padded)) | (slot > last)
        slot = jnp.where(none, -1, slot)
        found = jnp.where(lane == slot, inverse, 0)
        return jnp.sum(found, axis=1, keepdims=True) - 1

    shared = (group * length) % width == 0
    unroll = n_line <= 8
    wants = [wanted(step) for step in range(n_line)] if unroll else None

    def values(block, step):
        offset = base_of(step) % width
        turned = pltpu.roll(block, (width - offset) % width, 1)
        return jnp.transpose(turned)[:padded]

    def piece(slot, step, first, block, key_row, flat):
        want = wants[step] if unroll else wanted(step)
        if flat is None:
            flat = values(block, step)
        flat = jnp.concatenate([flat, jnp.ones((TAIL, nrows), jnp.float32)], axis=0)
        picked = jnp.where(key_row == want, flat, 0.0)
        gram = jnp.dot(
            picked, block, precision=lax.Precision.HIGHEST, preferred_element_type=jnp.float32
        )
        count = jnp.sum(picked[padded:], axis=1, keepdims=True)
        tail_row = lax.broadcasted_iota(jnp.int32, (TAIL, width), 0)
        tail = jnp.where(tail_row < TAIL // 2, gram[padded:], count)
        if first:
            part[step, :padded] = gram[:padded]
            part[step, padded:] = tail
        else:
            part[step, :padded] += gram[:padded]
            part[step, padded:] += tail

    def line_copy(step):
        return pltpu.make_async_remote_copy(
            src_ref=part.at[step], dst_ref=arrived.at[step],
            send_sem=line_send.at[step], recv_sem=line_recv.at[step],
            device_id=along(step), device_id_type=MESH,
        )

    def compute(slot, first=False, final=False):
        block = blocks[slot]
        key_row = jnp.concatenate(
            [keys[slot, i : i + 1, :] for i in range(nrows // LANES)], axis=1
        )
        flat = values(block, 0) if shared else None
        if unroll:
            for step in list(range(1, n_line)) + [0]:
                piece(slot, step, first, block, key_row, flat)
                if final and step:
                    line_copy(step).start()
        else:
            def body(step, c):
                piece(slot, step, first, block, key_row, flat)
                return c
            lax.fori_loop(0, n_line, body, 0)
            if final:
                def send(step, c):
                    line_copy(step).start()
                    return c
                lax.fori_loop(1, n_line, send, 0)

    def copies(src, dst, device, index):
        return [
            pltpu.make_async_remote_copy(
                src_ref=buf.at[src], dst_ref=buf.at[dst],
                send_sem=send_sem.at[i, index], recv_sem=recv_sem.at[i, dst],
                device_id=device, device_id_type=MESH,
            )
            for i, buf in enumerate((keys, blocks))
        ]

    for copy in loads:
        copy.wait()
    n_meet = len(far) + n_line
    pl.semaphore_wait(barrier, n_meet)

    sent = []

    def send(src, dst, device):
        for copy in copies(src, dst, device, len(sent)):
            copy.start()
        sent.append((src, dst, device, len(sent)))

    def receive(slot):
        for copy in copies(slot, slot, peer(1), 0):
            copy.wait_recv()

    for mask in far:
        send(0, mask, peer(mask))
    send(0, 1, peer(1))
    compute(0, first=True)
    receive(1)
    compute(1)
    near = far[:-1]
    for mask in near:
        receive(mask)
        send(mask, mask ^ 1, peer(1))
    for mask in near:
        compute(mask)
    for mask in near:
        receive(mask ^ 1)
        compute(mask ^ 1)
    for mask in far[-1:]:
        receive(mask)
        send(mask, mask ^ 1, peer(1))
        compute(mask)
        receive(mask ^ 1)
        compute(mask ^ 1, final=True)

    def collect(step, total):
        line_copy(step).wait_recv()
        return total + arrived[step]

    total = part[0]
    if unroll:
        for step in range(1, n_line):
            total = collect(step, total)
    else:
        total = lax.fori_loop(1, n_line, collect, total)

    base = base_of(0)
    index = lax.broadcasted_iota(jnp.int32, (padded, width), 0)
    column = lax.broadcasted_iota(jnp.int32, (padded, width), 1)
    flat_row = base + index
    segment = flat_row // width - base // width
    half = TAIL // 2
    sums = total[padded : padded + 1]
    count = total[padded + half : padded + half + 1]
    sums = jnp.broadcast_to(sums, (padded, width))
    count = jnp.broadcast_to(count, (padded, width))
    for s in range(1, half):
        sums = jnp.where(segment == s, total[padded + s : padded + s + 1], sums)
        count = jnp.where(segment == s, total[padded + half + s : padded + half + s + 1], count)
    own = jnp.sum(jnp.where(column == flat_row % width, sums, 0.0), axis=1, keepdims=True)
    result = (total[:padded] - own * sums / count) / (count - 1.0)
    out_ref[...] = result[:length]

    for item in sent:
        for copy in copies(*item):
            copy.wait_send()
    if unroll:
        for step in range(1, n_line):
            line_copy(step).wait_send()
    else:
        def drain(step, c):
            line_copy(step).wait_send()
            return c
        lax.fori_loop(1, n_line, drain, 0)


def solution(mesh):
    n_rows, n_grp = mesh.shape["rows"], mesh.shape["grp"]
    inner = 2
    group = inner * n_grp

    def local(features, key_ids, owner):
        nkeys = owner.shape[0]
        rows, width = features.shape
        length = nkeys * width // (n_rows * n_grp)
        padded = -(-length // 8) * 8
        n_line = n_rows // inner
        assert padded <= width == LANES and nkeys <= LANES and group & (group - 1) == 0
        keys = key_ids.reshape(rows // LANES, LANES)
        n_sent = group
        return pl.pallas_call(
            functools.partial(kernel, inner, n_grp, n_line, nkeys, length, padded),
            out_shape=jax.ShapeDtypeStruct((length, width), jnp.float32),
            in_specs=[
                pl.BlockSpec(memory_space=pltpu.MemorySpace.HBM),
                pl.BlockSpec(memory_space=pltpu.MemorySpace.HBM),
                pl.BlockSpec(memory_space=pltpu.MemorySpace.SMEM),
            ],
            out_specs=pl.BlockSpec(memory_space=pltpu.MemorySpace.VMEM),
            scratch_shapes=[
                pltpu.VMEM((group, rows, width), jnp.float32),
                pltpu.VMEM((group, rows // LANES, LANES), jnp.int32),
                pltpu.VMEM((n_line, padded + TAIL, width), jnp.float32),
                pltpu.VMEM((n_line, padded + TAIL, width), jnp.float32),
                pltpu.SemaphoreType.DMA((2,)),
                pltpu.SemaphoreType.DMA((2, n_sent)),
                pltpu.SemaphoreType.DMA((2, group)),
                pltpu.SemaphoreType.DMA((n_line,)),
                pltpu.SemaphoreType.DMA((n_line,)),
            ],
            compiler_params=pltpu.CompilerParams(collective_id=0, has_side_effects=True),
        )(features, keys, owner)

    placed = (P(("rows", "grp"), None), P(("rows", "grp")), P())
    return jax.shard_map(
        local, mesh=mesh, in_specs=placed, out_specs=P(("rows", "grp"), None), check_vma=False
    )
```

```python
import functools

import jax
import jax.numpy as jnp
from jax import lax
from jax.experimental import pallas as pl
from jax.experimental.pallas import tpu as pltpu
from jax.sharding import PartitionSpec as P

MESH = pl.DeviceIdType.MESH
LANES = 128
TAIL = 8


def flip(q, mask):
    bit = 1
    while bit <= mask:
        if mask & bit:
            q = q + bit * (1 - 2 * ((q // bit) % 2))
        bit *= 2
    return q


def kernel(
    inner, n_grp, n_line, nkeys, length, padded,
    feat_ref, key_ref, owner_ref, out_ref,
    owner_smem, blocks, keys, part, arrived, load_sem, send_sem, recv_sem, key_send, key_recv,
    line_send, line_recv,
):
    group = inner * n_grp
    nrows, width = feat_ref.shape
    r, g = lax.axis_index("rows"), lax.axis_index("grp")
    line = r // inner
    q = (r % inner) * n_grp + g

    def peer(mask):
        other = flip(q, mask)
        return (line * inner + other // n_grp, other % n_grp)

    def along(step):
        return (((line + step) % n_line) * inner + r % inner, g)

    loads = [
        pltpu.make_async_copy(feat_ref, blocks.at[0], load_sem.at[0]),
        pltpu.make_async_copy(key_ref, keys.at[0], load_sem.at[1]),
        pltpu.make_async_copy(owner_ref, owner_smem, load_sem.at[2]),
    ]
    for copy in loads:
        copy.start()
    barrier = pltpu.get_barrier_semaphore()
    for mask in range(1, group):
        pl.semaphore_signal(barrier, inc=1, device_id=peer(mask), device_id_type=MESH)
    if n_line <= 8:
        for step in range(1, n_line):
            pl.semaphore_signal(barrier, inc=1, device_id=along(step), device_id_type=MESH)
    else:
        def greet(step, c):
            pl.semaphore_signal(barrier, inc=1, device_id=along(step), device_id_type=MESH)
            return c
        lax.fori_loop(1, n_line, greet, 0)

    for copy in loads:
        copy.wait()

    lane = lax.broadcasted_iota(jnp.int32, (1, LANES), 1)
    inverse = jnp.zeros((1, LANES), jnp.int32)
    for k in range(nkeys):
        inverse = jnp.where(lane == owner_smem[k], k + 1, inverse)
    row = lax.broadcasted_iota(jnp.int32, (padded + TAIL, 1), 0)

    def base_of(step):
        return (((line + step) % n_line) * group + q) * length

    def wanted(step):
        base = base_of(step)
        tail = (row - padded) % (TAIL // 2)
        slot = jnp.where(row < padded, (base + row) // width, base // width + tail)
        last = (base + length - 1) // width
        none = ((row >= length) & (row < padded)) | (slot > last)
        slot = jnp.where(none, -1, slot)
        found = jnp.where(lane == slot, inverse, 0)
        return jnp.sum(found, axis=1, keepdims=True) - 1

    shared = (group * length) % width == 0
    unroll = n_line <= 8
    wants = [wanted(step) for step in range(n_line)] if unroll else None

    def values(block, step):
        offset = base_of(step) % width
        turned = pltpu.roll(block, (width - offset) % width, 1)
        return jnp.transpose(turned)[:padded]

    def halves(value):
        high = value.astype(jnp.bfloat16)
        return high, (value - high.astype(jnp.float32)).astype(jnp.bfloat16)

    def with_ones(flat):
        high, low = halves(jnp.concatenate([flat, jnp.ones((TAIL, nrows), jnp.float32)], axis=0))
        return jnp.concatenate([high, low], axis=1)

    def piece(step, first, block, right, key_row, left):
        want = wants[step] if unroll else wanted(step)
        if left is None:
            left = with_ones(values(block, step))
        mask = jnp.where(key_row == want, 1.0, 0.0)
        mask16 = mask.astype(jnp.bfloat16)
        picked = left * jnp.concatenate([mask16, mask16], axis=1)
        gram = jnp.dot(picked, right, preferred_element_type=jnp.float32)
        gram = gram[:, :width] + gram[:, width:]
        count = jnp.sum(mask[padded:], axis=1, keepdims=True)
        tail_row = lax.broadcasted_iota(jnp.int32, (TAIL, width), 0)
        tail = jnp.where(tail_row < TAIL // 2, gram[padded:], count)
        if first:
            part[step, :padded] = gram[:padded]
            part[step, padded:] = tail
        else:
            part[step, :padded] += gram[:padded]
            part[step, padded:] += tail

    def line_copy(step):
        return pltpu.make_async_remote_copy(
            src_ref=part.at[step], dst_ref=arrived.at[step],
            send_sem=line_send.at[step], recv_sem=line_recv.at[step],
            device_id=along(step), device_id_type=MESH,
        )

    def compute(slot, first=False, final=False):
        block = blocks[slot]
        key_row = jnp.concatenate(
            [keys[slot, i : i + 1, :] for i in range(nrows // LANES)], axis=1
        )
        right = jnp.concatenate(halves(block), axis=1)
        right = jnp.concatenate([right, right], axis=0)
        left = with_ones(values(block, 0)) if shared else None
        if unroll:
            for step in list(range(1, n_line)) + [0]:
                piece(step, first, block, right, key_row, left)
                if final and step:
                    line_copy(step).start()
        else:
            def body(step, c):
                piece(step, first, block, right, key_row, left)
                return c
            lax.fori_loop(0, n_line, body, 0)
            if final:
                def send(step, c):
                    line_copy(step).start()
                    return c
                lax.fori_loop(1, n_line, send, 0)

    half_rows = nrows // 2

    def half_copy(src, dst, half, device, index):
        rows = pl.ds(half * half_rows, half_rows)
        return pltpu.make_async_remote_copy(
            src_ref=blocks.at[src, rows], dst_ref=blocks.at[dst, rows],
            send_sem=send_sem.at[index], recv_sem=recv_sem.at[dst, half],
            device_id=device, device_id_type=MESH,
        )

    def key_copy(mask):
        return pltpu.make_async_remote_copy(
            src_ref=keys.at[0], dst_ref=keys.at[mask],
            send_sem=key_send.at[mask], recv_sem=key_recv.at[mask],
            device_id=peer(mask), device_id_type=MESH,
        )

    pl.semaphore_wait(barrier, group - 1 + n_line - 1)

    sent = []

    def send(src, dst, half, device):
        item = (src, dst, half, device, len(sent))
        half_copy(*item).start()
        sent.append(item)

    def receive(slot, half):
        half_copy(slot, slot, half, peer(1), 0).wait_recv()

    def hand_over(slot, half):
        send(slot, slot ^ 1, half, peer(1))

    def partner_block(slot):
        receive(slot, 0)
        receive(slot, 1)

    send(0, 2, 0, peer(2))
    send(0, 4, 1, peer(4))
    send(0, 2, 1, peer(2))
    send(0, 4, 0, peer(4))
    send(0, 1, 0, peer(1))
    send(0, 1, 1, peer(1))
    for mask in range(1, group):
        key_copy(mask).start()
    for mask in range(1, group):
        key_copy(mask).wait_recv()
    compute(0, first=True)
    partner_block(1)
    compute(1)
    receive(2, 0)
    send(2, 6, 0, peer(4))
    hand_over(2, 0)
    receive(4, 1)
    send(4, 6, 1, peer(2))
    hand_over(4, 1)
    receive(2, 1)
    hand_over(2, 1)
    receive(4, 0)
    hand_over(4, 0)
    compute(2)
    compute(4)
    partner_block(3)
    compute(3)
    partner_block(5)
    compute(5)
    receive(6, 0)
    hand_over(6, 0)
    receive(6, 1)
    hand_over(6, 1)
    compute(6)
    partner_block(7)
    compute(7, final=True)

    def collect(step, total):
        line_copy(step).wait_recv()
        return total + arrived[step]

    total = part[0]
    if unroll:
        for step in range(1, n_line):
            total = collect(step, total)
    else:
        total = lax.fori_loop(1, n_line, collect, total)

    base = base_of(0)
    index = lax.broadcasted_iota(jnp.int32, (padded, width), 0)
    column = lax.broadcasted_iota(jnp.int32, (padded, width), 1)
    flat_row = base + index
    segment = flat_row // width - base // width
    half = TAIL // 2
    sums = total[padded : padded + 1]
    count = total[padded + half : padded + half + 1]
    sums = jnp.broadcast_to(sums, (padded, width))
    count = jnp.broadcast_to(count, (padded, width))
    for s in range(1, half):
        sums = jnp.where(segment == s, total[padded + s : padded + s + 1], sums)
        count = jnp.where(segment == s, total[padded + half + s : padded + half + s + 1], count)
    own = jnp.sum(jnp.where(column == flat_row % width, sums, 0.0), axis=1, keepdims=True)
    result = (total[:padded] - own * sums / count) / (count - 1.0)
    out_ref[...] = result[:length]

    for item in sent:
        half_copy(*item).wait_send()
    for mask in range(1, group):
        key_copy(mask).wait_send()
    if unroll:
        for step in range(1, n_line):
            line_copy(step).wait_send()
    else:
        def drain(step, c):
            line_copy(step).wait_send()
            return c
        lax.fori_loop(1, n_line, drain, 0)


def solution(mesh):
    n_rows, n_grp = mesh.shape["rows"], mesh.shape["grp"]
    group = 8
    inner = group // n_grp
    assert inner * n_grp == group and n_rows % inner == 0

    def local(features, key_ids, owner):
        nkeys = owner.shape[0]
        rows, width = features.shape
        length = nkeys * width // (n_rows * n_grp)
        padded = -(-length // 8) * 8
        n_line = n_rows // inner
        assert padded <= width == LANES and nkeys <= LANES and rows % (2 * LANES) == 0
        keys = key_ids.reshape(rows // LANES, LANES)
        return pl.pallas_call(
            functools.partial(kernel, inner, n_grp, n_line, nkeys, length, padded),
            out_shape=jax.ShapeDtypeStruct((length, width), jnp.float32),
            in_specs=[
                pl.BlockSpec(memory_space=pltpu.MemorySpace.HBM),
                pl.BlockSpec(memory_space=pltpu.MemorySpace.HBM),
                pl.BlockSpec(memory_space=pltpu.MemorySpace.HBM),
            ],
            out_specs=pl.BlockSpec(memory_space=pltpu.MemorySpace.VMEM),
            scratch_shapes=[
                pltpu.SMEM((nkeys,), jnp.int32),
                pltpu.VMEM((group, rows, width), jnp.float32),
                pltpu.VMEM((group, rows // LANES, LANES), jnp.int32),
                pltpu.VMEM((n_line, padded + TAIL, width), jnp.float32),
                pltpu.VMEM((n_line, padded + TAIL, width), jnp.float32),
                pltpu.SemaphoreType.DMA((3,)),
                pltpu.SemaphoreType.DMA((2 * group - 2,)),
                pltpu.SemaphoreType.DMA((group, 2)),
                pltpu.SemaphoreType.DMA((group,)),
                pltpu.SemaphoreType.DMA((group,)),
                pltpu.SemaphoreType.DMA((n_line,)),
                pltpu.SemaphoreType.DMA((n_line,)),
            ],
            compiler_params=pltpu.CompilerParams(collective_id=0, has_side_effects=True),
        )(features, keys, owner)

    placed = (P(("rows", "grp"), None), P(("rows", "grp")), P())
    return jax.shard_map(
        local, mesh=mesh, in_specs=placed, out_specs=P(("rows", "grp"), None), check_vma=False
    )
```

```python
import functools

import jax
import jax.numpy as jnp
from jax import lax
from jax.experimental import pallas as pl
from jax.experimental.pallas import tpu as pltpu
from jax.sharding import PartitionSpec as P

MESH = pl.DeviceIdType.MESH
LANES = 128
TAIL = 8


def flip(q, mask):
    bit = 1
    while bit <= mask:
        if mask & bit:
            q = q + bit * (1 - 2 * ((q // bit) % 2))
        bit *= 2
    return q


def kernel(
    inner, n_grp, n_line, nkeys, length, padded,
    feat_ref, key_ref, owner_ref, out_ref,
    owner_smem, blocks, keys, part, arrived, load_sem, send_sem, recv_sem, key_send, key_recv,
    line_send, line_recv,
):
    group = inner * n_grp
    nrows, width = feat_ref.shape
    r, g = lax.axis_index("rows"), lax.axis_index("grp")
    line = r // inner
    q = (r % inner) * n_grp + g

    def peer(mask):
        other = flip(q, mask)
        return (line * inner + other // n_grp, other % n_grp)

    def along(step):
        return (((line + step) % n_line) * inner + r % inner, g)

    loads = [
        pltpu.make_async_copy(feat_ref, blocks.at[0], load_sem.at[0]),
        pltpu.make_async_copy(key_ref, keys.at[0], load_sem.at[1]),
        pltpu.make_async_copy(owner_ref, owner_smem, load_sem.at[2]),
    ]
    for copy in loads:
        copy.start()
    barrier = pltpu.get_barrier_semaphore()
    for mask in (1, 2, 4):
        pl.semaphore_signal(barrier, inc=1, device_id=peer(mask), device_id_type=MESH)
    if n_line <= 8:
        for step in range(1, n_line):
            pl.semaphore_signal(barrier, inc=1, device_id=along(step), device_id_type=MESH)
    else:
        def greet(step, c):
            pl.semaphore_signal(barrier, inc=1, device_id=along(step), device_id_type=MESH)
            return c
        lax.fori_loop(1, n_line, greet, 0)

    for copy in loads:
        copy.wait()

    lane = lax.broadcasted_iota(jnp.int32, (1, LANES), 1)
    inverse = jnp.zeros((1, LANES), jnp.int32)
    for k in range(nkeys):
        inverse = jnp.where(lane == owner_smem[k], k + 1, inverse)
    row = lax.broadcasted_iota(jnp.int32, (padded + TAIL, 1), 0)

    def base_of(step):
        return (((line + step) % n_line) * group + q) * length

    def wanted(step):
        base = base_of(step)
        tail = (row - padded) % (TAIL // 2)
        slot = jnp.where(row < padded, (base + row) // width, base // width + tail)
        last = (base + length - 1) // width
        none = ((row >= length) & (row < padded)) | (slot > last)
        slot = jnp.where(none, -1, slot)
        found = jnp.where(lane == slot, inverse, 0)
        return jnp.sum(found, axis=1, keepdims=True) - 1

    shared = (group * length) % width == 0
    unroll = n_line <= 8
    wants = [wanted(step) for step in range(n_line)] if unroll else None

    def values(block, step):
        offset = base_of(step) % width
        turned = pltpu.roll(block, (width - offset) % width, 1)
        return jnp.transpose(turned)[:padded]

    def halves(value):
        high = value.astype(jnp.bfloat16)
        return high, (value - high.astype(jnp.float32)).astype(jnp.bfloat16)

    def with_ones(flat):
        high, low = halves(jnp.concatenate([flat, jnp.ones((TAIL, nrows), jnp.float32)], axis=0))
        return jnp.concatenate([high, low], axis=1)

    def piece(step, first, block, right, key_row, left):
        want = wants[step] if unroll else wanted(step)
        if left is None:
            left = with_ones(values(block, step))
        mask = jnp.where(key_row == want, 1.0, 0.0)
        mask16 = mask.astype(jnp.bfloat16)
        picked = left * jnp.concatenate([mask16, mask16], axis=1)
        gram = jnp.dot(picked, right, preferred_element_type=jnp.float32)
        gram = gram[:, :width] + gram[:, width:]
        count = jnp.sum(mask[padded:], axis=1, keepdims=True)
        tail_row = lax.broadcasted_iota(jnp.int32, (TAIL, width), 0)
        tail = jnp.where(tail_row < TAIL // 2, gram[padded:], count)
        if first:
            part[step, :padded] = gram[:padded]
            part[step, padded:] = tail
        else:
            part[step, :padded] += gram[:padded]
            part[step, padded:] += tail

    def line_copy(step):
        return pltpu.make_async_remote_copy(
            src_ref=part.at[step], dst_ref=arrived.at[step],
            send_sem=line_send.at[step], recv_sem=line_recv.at[step],
            device_id=along(step), device_id_type=MESH,
        )

    def compute(slot, first=False, final=False):
        block = blocks[slot]
        key_row = jnp.concatenate(
            [keys[slot, i : i + 1, :] for i in range(nrows // LANES)], axis=1
        )
        right = jnp.concatenate(halves(block), axis=1)
        right = jnp.concatenate([right, right], axis=0)
        left = with_ones(values(block, 0)) if shared else None
        if unroll:
            for step in list(range(1, n_line)) + [0]:
                piece(step, first, block, right, key_row, left)
                if final and step:
                    line_copy(step).start()
        else:
            def body(step, c):
                piece(step, first, block, right, key_row, left)
                return c
            lax.fori_loop(0, n_line, body, 0)
            if final:
                def send(step, c):
                    line_copy(step).start()
                    return c
                lax.fori_loop(1, n_line, send, 0)

    half_rows = nrows // 2

    def key_copy(src, dst, device):
        return pltpu.make_async_remote_copy(
            src_ref=keys.at[src], dst_ref=keys.at[dst],
            send_sem=key_send.at[dst], recv_sem=key_recv.at[dst],
            device_id=device, device_id_type=MESH,
        )

    def half_copy(src, dst, half, device, index):
        rows = pl.ds(half * half_rows, half_rows)
        return pltpu.make_async_remote_copy(
            src_ref=blocks.at[src, rows], dst_ref=blocks.at[dst, rows],
            send_sem=send_sem.at[index], recv_sem=recv_sem.at[dst, half],
            device_id=device, device_id_type=MESH,
        )

    pl.semaphore_wait(barrier, 3 + n_line - 1)

    sent = []

    def send(src, dst, half, device):
        item = (src, dst, half, device, len(sent))
        if half == 0:
            key_copy(src, dst, device).start()
        half_copy(*item).start()
        sent.append(item)

    def receive(slot, half):
        if half == 0:
            key_copy(slot, slot, peer(1)).wait_recv()
        half_copy(slot, slot, half, peer(1), 0).wait_recv()

    def hand_over(slot, half):
        send(slot, slot ^ 1, half, peer(1))

    def partner_block(slot):
        receive(slot, 0)
        receive(slot, 1)

    send(0, 2, 0, peer(2))
    send(0, 4, 1, peer(4))
    send(0, 2, 1, peer(2))
    send(0, 4, 0, peer(4))
    send(0, 1, 0, peer(1))
    send(0, 1, 1, peer(1))
    compute(0, first=True)
    partner_block(1)
    compute(1)
    receive(2, 0)
    send(2, 6, 0, peer(4))
    hand_over(2, 0)
    receive(4, 1)
    send(4, 6, 1, peer(2))
    hand_over(4, 1)
    receive(2, 1)
    hand_over(2, 1)
    receive(4, 0)
    hand_over(4, 0)
    compute(2)
    compute(4)
    partner_block(3)
    compute(3)
    partner_block(5)
    compute(5)
    receive(6, 0)
    hand_over(6, 0)
    receive(6, 1)
    hand_over(6, 1)
    compute(6)
    partner_block(7)
    compute(7, final=True)

    def collect(step, total):
        line_copy(step).wait_recv()
        return total + arrived[step]

    total = part[0]
    if unroll:
        for step in range(1, n_line):
            total = collect(step, total)
    else:
        total = lax.fori_loop(1, n_line, collect, total)

    base = base_of(0)
    index = lax.broadcasted_iota(jnp.int32, (padded, width), 0)
    column = lax.broadcasted_iota(jnp.int32, (padded, width), 1)
    flat_row = base + index
    segment = flat_row // width - base // width
    half = TAIL // 2
    sums = total[padded : padded + 1]
    count = total[padded + half : padded + half + 1]
    sums = jnp.broadcast_to(sums, (padded, width))
    count = jnp.broadcast_to(count, (padded, width))
    for s in range(1, half):
        sums = jnp.where(segment == s, total[padded + s : padded + s + 1], sums)
        count = jnp.where(segment == s, total[padded + half + s : padded + half + s + 1], count)
    own = jnp.sum(jnp.where(column == flat_row % width, sums, 0.0), axis=1, keepdims=True)
    result = (total[:padded] - own * sums / count) / (count - 1.0)
    out_ref[...] = result[:length]

    for item in sent:
        half_copy(*item).wait_send()
    for item in sent:
        if item[2] == 0:
            key_copy(item[0], item[1], item[3]).wait_send()
    if unroll:
        for step in range(1, n_line):
            line_copy(step).wait_send()
    else:
        def drain(step, c):
            line_copy(step).wait_send()
            return c
        lax.fori_loop(1, n_line, drain, 0)


def solution(mesh):
    n_rows, n_grp = mesh.shape["rows"], mesh.shape["grp"]
    group = 8
    inner = group // n_grp
    assert inner * n_grp == group and n_rows % inner == 0

    def local(features, key_ids, owner):
        nkeys = owner.shape[0]
        rows, width = features.shape
        length = nkeys * width // (n_rows * n_grp)
        padded = -(-length // 8) * 8
        n_line = n_rows // inner
        assert padded <= width == LANES and nkeys <= LANES and rows % (2 * LANES) == 0
        keys = key_ids.reshape(rows // LANES, LANES)
        return pl.pallas_call(
            functools.partial(kernel, inner, n_grp, n_line, nkeys, length, padded),
            out_shape=jax.ShapeDtypeStruct((length, width), jnp.float32),
            in_specs=[
                pl.BlockSpec(memory_space=pltpu.MemorySpace.HBM),
                pl.BlockSpec(memory_space=pltpu.MemorySpace.HBM),
                pl.BlockSpec(memory_space=pltpu.MemorySpace.HBM),
            ],
            out_specs=pl.BlockSpec(memory_space=pltpu.MemorySpace.VMEM),
            scratch_shapes=[
                pltpu.SMEM((nkeys,), jnp.int32),
                pltpu.VMEM((group, rows, width), jnp.float32),
                pltpu.VMEM((group, rows // LANES, LANES), jnp.int32),
                pltpu.VMEM((n_line, padded + TAIL, width), jnp.float32),
                pltpu.VMEM((n_line, padded + TAIL, width), jnp.float32),
                pltpu.SemaphoreType.DMA((3,)),
                pltpu.SemaphoreType.DMA((2 * group - 2,)),
                pltpu.SemaphoreType.DMA((group, 2)),
                pltpu.SemaphoreType.DMA((group,)),
                pltpu.SemaphoreType.DMA((group,)),
                pltpu.SemaphoreType.DMA((n_line,)),
                pltpu.SemaphoreType.DMA((n_line,)),
            ],
            compiler_params=pltpu.CompilerParams(collective_id=0, has_side_effects=True),
        )(features, keys, owner)

    placed = (P(("rows", "grp"), None), P(("rows", "grp")), P())
    return jax.shard_map(
        local, mesh=mesh, in_specs=placed, out_specs=P(("rows", "grp"), None), check_vma=False
    )
```
